128 devices in a mesh: seq: 2 (over z_lo), ctx: 8 (over y, core), exp: 8 (over z_hi, x).
Axes of the slice: x: 4, y: 4, z: 4 (z_hi: 2, z_lo: 2; z = z_hi * 2 + z_lo), core: 2. Of those that a mesh axis runs over, the one named last changes fastest.
Arguments:
- tokens: bfloat16 [2, 8192, 7168], P('seq', ('ctx', 'exp')), may hold values from -8 to 8
- routing: int32 [2, 8192, 8], P('seq', ('ctx', 'exp')), may hold values from 0 to 255, as said below
- router_weight: bfloat16 [7168, 256], replicated, may hold values from -0.0625 to 0.0625
- w_gate: bfloat16 [16, 7168, 2048], P(('seq', 'exp'), None, 'ctx'), may hold values from -0.0625 to 0.0625
- w_up: bfloat16 [16, 7168, 2048], P(('seq', 'exp'), None, 'ctx'), may hold values from -0.0625 to 0.0625
- w_down: bfloat16 [16, 2048, 7168], P(('seq', 'exp'), 'ctx'), may hold values from -0.125 to 0.125
Outputs:
- routed: bfloat16 [2, 8192, 7168], P('seq', ('ctx', 'exp'))
- balance: float32 [2, 256], P('seq')
The draws below stay inside these ranges and needn't reach their ends.
Inputs may be any that keep to these rules, and one draw needn't show every extreme that they name: `routing`: each token names 8 different experts. The rows of one device name any one expert at least 3 and at most 5 times; in every draw one expert below 16 is named exactly 5 times by the rows of every device.
All inputs are finite; a program needn't handle non-finite values.
Results may differ from the reference program's by a relative error of at most 0.014.
Values may be sent and summed in bfloat16 or wider, within the bound.
No kernel may reach another device: no remote copies, remote signals or barrier semaphores. Data moves between devices by JAX's collectives and lax.ppermute only.
A program may use at most 128 MiB of HBM per device.

```python
import jax
import jax.numpy as jnp
from jax import lax

D = 7168
FF = 2048
EXPERTS = 256
TOP = 8
TOK_DEV = 128
FLIGHT = 16
SEQS = 2
LENGTH = 8192
CAPACITY = 5
N_SEQ = 2
N_CTX = 8
N_EXP = 8


def draw_tokens(key, part):
    key_jitter, key_direction = jax.random.split(key, 2)
    positions = jnp.arange(LENGTH, dtype=jnp.float32) / (LENGTH - 1)
    direction = jax.random.normal(key_direction, (SEQS, 1, D), jnp.float32)
    jitter_part = jax.random.normal(key_jitter, (SEQS, LENGTH, D), jnp.float32)
    strength = 0.3 + 0.6 * positions
    values = jitter_part + strength[None, :, None] * direction
    return jnp.clip(values, -8.0, 8.0).astype(jnp.bfloat16)


def draw_routing(key, part):
    blocks = SEQS * LENGTH // TOK_DEV
    classes = EXPERTS // TOP
    mean_load = TOK_DEV * TOP // EXPERTS
    reach = mean_load // 4
    key_pick, key_shift, key_order, key_lift, key_perm = jax.random.split(key, 5)
    full_expert = jax.random.randint(key_pick, (), 0, FLIGHT).astype(jnp.int32)
    shifts = jax.random.randint(key_shift, (blocks, classes // 2), -reach, reach + 1).astype(jnp.int32)
    shifts = shifts.at[:, 0].set(reach)
    counts = jnp.stack([mean_load + shifts, mean_load - shifts], axis=2).reshape(blocks, classes)
    bounds = jnp.cumsum(counts, axis=1).astype(jnp.int32)
    ranks = jnp.arange(TOK_DEV, dtype=jnp.int32)
    class_of_rank = jnp.sum((ranks[None, :, None] >= bounds[:, None, :]).astype(jnp.int32), axis=2).astype(jnp.int32)
    orders = jax.vmap(lambda sub: jax.random.permutation(sub, TOK_DEV))(jax.random.split(key_order, blocks)).astype(jnp.int32)
    token_class = jnp.take_along_axis(class_of_rank, orders, axis=1)
    lifts = jax.random.randint(key_lift, (blocks, TOK_DEV), 0, TOP).astype(jnp.int32)
    base = token_class + classes * lifts
    perms = jax.vmap(lambda sub: jax.random.permutation(sub, EXPERTS))(jax.random.split(key_perm, blocks)).astype(jnp.int32)
    where_full = jnp.argmax(perms == full_expert, axis=1).astype(jnp.int32)
    first_entry = perms[:, 0]
    positions = jnp.arange(EXPERTS, dtype=jnp.int32)[None, :]
    perms = jnp.where(positions == 0, full_expert, jnp.where(positions == where_full[:, None], first_entry[:, None], perms))
    offsets = jnp.arange(TOP, dtype=jnp.int32) * classes
    picks = (base[:, :, None] + offsets[None, None, :]) % EXPERTS
    chosen = jnp.take_along_axis(perms, picks.reshape(blocks, TOK_DEV * TOP), axis=1)
    return chosen.reshape(SEQS, LENGTH, TOP).astype(jnp.int32)


def block_scale(stream_key, dims, cuts, low, top_value):
    def one(position, shards_of):
        steps = jax.random.uniform(jax.random.fold_in(jax.random.fold_in(stream_key, 6), position), (shards_of,), jnp.float32, low / len(cuts), top_value / len(cuts))
        return jnp.repeat(jnp.exp(steps), dims[position] // shards_of).reshape((-1,) + (1,) * (len(dims) - position - 1))

    factor_of = one(*cuts[0])
    for cut in cuts[1:]:
        factor_of = factor_of * one(*cut)
    return factor_of


def scatter_about(stream_key, shape, width, most, shards=(), kind=jnp.bfloat16):
    factor_of = block_scale(stream_key, shape, shards, -0.22, 0.18) if shards else 1.0
    drawn = jax.random.normal(stream_key, shape, jnp.float32) * width * factor_of
    return jnp.minimum(jnp.maximum(drawn, -most), most).astype(kind)


def setup_inputs(seed: int = 0) -> dict:
    splits = jax.random.split(jax.random.key(seed), 7)
    tokens = draw_tokens(jax.random.fold_in(splits[6], 71), 0)
    routing = draw_routing(jax.random.fold_in(splits[6], 71), 0)
    router_weight = scatter_about(splits[2], (D, EXPERTS), D ** -0.5, 0.0625)
    w_gate = scatter_about(splits[3], (FLIGHT, D, FF), D ** -0.5, 0.0625, ((0, 16), (2, 8)))
    w_up = scatter_about(splits[4], (FLIGHT, D, FF), D ** -0.5, 0.0625, ((0, 16), (2, 8)))
    w_down = scatter_about(splits[5], (FLIGHT, FF, D), FF ** -0.5, 0.125, ((0, 16), (1, 8)))
    return dict(tokens=tokens, routing=routing, router_weight=router_weight, w_gate=w_gate, w_up=w_up, w_down=w_down)


route_scale = 2.5


def expert_block(row_block, gate_weight, up_weight, down_weight):
    gate_proj = jnp.dot(row_block, gate_weight, preferred_element_type=jnp.float32)
    up_proj = jnp.dot(row_block, up_weight, preferred_element_type=jnp.float32)
    hidden = (jax.nn.silu(gate_proj) * up_proj).astype(jnp.bfloat16)
    block_width = FF // N_CTX
    combined = jnp.zeros((row_block.shape[0], D), jnp.float32)
    for column in range(N_CTX):
        lower = column * block_width
        partial_value = jnp.dot(hidden[:, lower:lower + block_width], down_weight[lower:lower + block_width], preferred_element_type=jnp.float32)
        rounded = lax.optimization_barrier(partial_value.astype(jnp.bfloat16))
        combined = combined + rounded.astype(jnp.float32)
    return combined.astype(jnp.bfloat16)


def reference(tokens, routing, router_weight, w_gate, w_up, w_down):
    flight = N_SEQ * N_EXP
    blocks = SEQS * LENGTH // TOK_DEV
    per_block = TOK_DEV * TOP
    flat_tokens = tokens.reshape(SEQS * LENGTH, D)
    routes = routing.reshape(SEQS * LENGTH, TOP)
    logits = jnp.dot(flat_tokens, router_weight, preferred_element_type=jnp.float32)
    scores = jax.nn.sigmoid(logits)
    affinity = scores / jnp.sum(scores, axis=1, keepdims=True)
    picked = jnp.take_along_axis(scores, routes, axis=1)
    gate_weights = picked / jnp.sum(picked, axis=1, keepdims=True) * route_scale
    prob_sum = jnp.sum(affinity.reshape(SEQS, LENGTH, EXPERTS), axis=1)
    seq_of_row = (jnp.arange(SEQS * LENGTH, dtype=jnp.int32) // LENGTH)[:, None]
    load = jnp.zeros((SEQS, EXPERTS), jnp.float32).at[jnp.broadcast_to(seq_of_row, routes.shape), routes].add(1.0)
    balance = load * (EXPERTS / (TOP * LENGTH)) * (prob_sum / LENGTH) * EXPERTS

    block_routes = routes.reshape(blocks, per_block)
    expert_iota = jnp.arange(flight, dtype=jnp.int32)[None, None, :]
    onehot = (block_routes[:, :, None] == expert_iota).astype(jnp.int32)
    slot_rank = jnp.sum((jnp.cumsum(onehot, axis=1) - onehot) * onehot, axis=2)
    is_live = block_routes < flight
    block_ids = jnp.arange(blocks, dtype=jnp.int32)[:, None]
    row_index = block_routes * (blocks * CAPACITY) + block_ids * CAPACITY + slot_rank
    spare = flight * blocks * CAPACITY
    target = jnp.where(is_live, row_index, spare)
    owner = block_ids * TOK_DEV + jnp.arange(per_block, dtype=jnp.int32)[None, :] // TOP
    source_row = jnp.zeros((spare + 1,), jnp.int32).at[target.reshape(-1)].set(owner.reshape(-1))
    filled = jnp.zeros((spare + 1,), jnp.int32).at[target.reshape(-1)].set(1)
    source_row = source_row[:spare].reshape(flight, blocks * CAPACITY)
    filled = filled[:spare].reshape(flight, blocks * CAPACITY)

    def one_expert(inputs):
        rows_of, filled_of, gate_weight, up_weight, down_weight = inputs
        row_block = jnp.where(filled_of[:, None] > 0, flat_tokens[rows_of], jnp.zeros((), flat_tokens.dtype))
        return expert_block(row_block, gate_weight, up_weight, down_weight)

    expert_out = lax.map(one_expert, (source_row, filled, w_gate, w_up, w_down))
    expert_out = expert_out.reshape(spare, D)
    live_gates = jnp.where(is_live, gate_weights.reshape(blocks, per_block), 0.0).reshape(SEQS * LENGTH, TOP)
    gather_index = jnp.where(is_live, row_index, 0).reshape(SEQS * LENGTH, TOP)
    combined = jnp.zeros((SEQS * LENGTH, D), jnp.float32)
    for column in range(TOP):
        combined = combined + live_gates[:, column:column + 1] * expert_out[gather_index[:, column]]
    routed = combined.astype(jnp.bfloat16).reshape(SEQS, LENGTH, D)
    return routed, balance
```

```python
import jax
import jax.numpy as jnp
from jax import lax
from jax.sharding import PartitionSpec as P

route_scale = 2.5
CHUNKS = (2, 3)
XZ = ("seq", "exp")


def swap_cores(array):
    size = lax.axis_size("ctx")
    return lax.ppermute(array, "ctx", [(i, i ^ 1) for i in range(size)])


def along_y(array, step):
    size = lax.axis_size("ctx")
    return lax.ppermute(array, "ctx", [(i, (i + 2 * step) % size) for i in range(size)])


def copy_for_each(array, axis):
    copies = jnp.broadcast_to(array, (lax.axis_size(axis), *array.shape))
    return lax.all_to_all(copies, axis, split_axis=0, concat_axis=0, tiled=True)


def f32_dot(a, b):
    return jnp.dot(a, b, preferred_element_type=jnp.float32)


def add_up(*arrays):
    total = arrays[0].astype(jnp.float32)
    for a in arrays[1:]:
        total = total + a.astype(jnp.float32)
    return total.astype(jnp.bfloat16)


def on_device(tokens, routing, router_weight, w_gate, w_up, w_down):
    token_rows = tokens[0]
    routes = routing[0]
    token_count, width = token_rows.shape
    top_count = routes.shape[1]
    experts = router_weight.shape[1]
    flight = lax.axis_size("seq") * lax.axis_size("exp")
    length = token_count * lax.axis_size("ctx") * lax.axis_size("exp")
    lanes = 128
    folds = width // lanes

    gates = (w_gate[0], swap_cores(w_gate[0]))
    ups = (w_up[0], swap_cores(w_up[0]))
    downs = (w_down[0], swap_cores(w_down[0]))

    routes_t = routes.T
    upper = (
        lax.broadcasted_iota(jnp.int32, (token_count, token_count), 0)
        < lax.broadcasted_iota(jnp.int32, (token_count, token_count), 1)
    ).astype(jnp.bfloat16)

    picks = []
    first = 0
    for n in CHUNKS:
        row = lax.broadcasted_iota(jnp.int32, (flight * n, 1), 0)
        expert_of, slot_of = row // n, first + row % n
        named = jnp.zeros((flight * n, token_count), jnp.bfloat16)
        for k in range(top_count):
            named = named + (routes_t[k][None, :] == expert_of).astype(jnp.bfloat16)
        rank = f32_dot(named, upper)
        picks.append(jnp.where(rank == slot_of.astype(jnp.float32), named, jnp.zeros((), jnp.bfloat16)))
        first += n

    half = flight // 2
    blocks = []
    for n, pick in zip(CHUNKS, picks):
        out = f32_dot(pick, token_rows).astype(jnp.bfloat16)
        out = out.reshape(flight, n * folds, lanes)
        mine = lax.all_to_all(out, XZ, split_axis=0, concat_axis=0, tiled=True)
        below = along_y(mine, 1)
        above = along_y(mine, -1)
        far_a = along_y(below[:half], 1)
        far_b = along_y(above[half:], -1)
        blocks.append((mine, below, above, far_a, far_b))

    returned = []
    for n, parts in zip(CHUNKS, blocks):
        rows = jnp.concatenate(parts).reshape(4 * flight * n, width)
        hidden = [
            (jax.nn.silu(f32_dot(rows, g)) * f32_dot(rows, u)).astype(jnp.bfloat16) for g, u in zip(gates, ups)
        ]
        part = (f32_dot(hidden[0], downs[0]) + f32_dot(hidden[1], downs[1])).astype(jnp.bfloat16)
        part = part.reshape(4, flight, n * folds, lanes)
        got_a = along_y(part[3, :half], 1)
        got_b = along_y(part[3, half:], -1)
        to_above = jnp.concatenate([add_up(part[2, :half], got_a), part[2, half:]])
        to_below = jnp.concatenate([part[1, :half], add_up(part[1, half:], got_b)])
        from_below = along_y(to_above, 1)
        from_above = along_y(to_below, -1)
        total = add_up(part[0], from_below, from_above)
        back = lax.all_to_all(total, XZ, split_axis=0, concat_axis=0, tiled=True)
        returned.append(back.reshape(flight * n, width))

    scores = jax.nn.sigmoid(f32_dot(token_rows, router_weight))
    affinity = scores / jnp.sum(scores, axis=1, keepdims=True)
    expert_iota = lax.broadcasted_iota(jnp.int32, (1, experts), 1)
    chosen = jnp.zeros((token_count, experts), jnp.float32)
    for k in range(top_count):
        chosen = chosen + (routes[:, k : k + 1] == expert_iota).astype(jnp.float32)
    gate_table = scores / jnp.sum(scores * chosen, axis=1, keepdims=True) * route_scale
    stats = jnp.concatenate([jnp.sum(affinity, axis=0), jnp.sum(chosen, axis=0)])
    stats = copy_for_each(stats, ("ctx", "exp")).reshape(-1, 2 * experts).sum(axis=0)
    prob_sum, load_sum = stats[:experts], stats[experts:]
    balance = load_sum * (experts / (top_count * length)) * (prob_sum / length) * experts

    combined = jnp.zeros((token_count, width), jnp.float32)
    for n, pick, back in zip(CHUNKS, picks, returned):
        spread = (
            lax.broadcasted_iota(jnp.int32, (flight, flight * n), 0)
            == lax.broadcasted_iota(jnp.int32, (flight, flight * n), 1) // n
        ).astype(jnp.float32)
        weight = jnp.dot(gate_table[:, :flight], spread, precision=lax.Precision.HIGHEST) * pick.T.astype(jnp.float32)
        high = weight.astype(jnp.bfloat16)
        low = (weight - high.astype(jnp.float32)).astype(jnp.bfloat16)
        combined = combined + f32_dot(high, back) + f32_dot(low, back)
    return (combined.astype(jnp.bfloat16)[None], balance[None])


def solution(mesh):
    placed = (
        P("seq", ("ctx", "exp"), None),
        P("seq", ("ctx", "exp"), None),
        P(),
        P(("seq", "exp"), None, "ctx"),
        P(("seq", "exp"), None, "ctx"),
        P(("seq", "exp"), "ctx", None),
    )
    return jax.shard_map(
        on_device,
        mesh=mesh,
        in_specs=placed,
        out_specs=(P("seq", ("ctx", "exp"), None), P("seq", None)),
        check_vma=False,
    )
```

```python
import functools

import jax
import jax.numpy as jnp
from jax import lax
from jax.experimental import pallas as pl
from jax.experimental.pallas import tpu as pltpu
from jax.sharding import PartitionSpec as P

route_scale = 2.5
CHUNKS = (2, 3)
XZ = ("seq", "exp")


def swap_cores(array):
    size = lax.axis_size("ctx")
    return lax.ppermute(array, "ctx", [(i, i ^ 1) for i in range(size)])


def ring(array):
    size = lax.axis_size("ctx")
    return lax.ppermute(array, "ctx", [(i, (i + 2 if i % 2 == 0 else i - 2) % size) for i in range(size)])


def sum_all(array):
    for axis in ("ctx", "exp"):
        size, bit = lax.axis_size(axis), 1
        while bit < size:
            array = array + lax.ppermute(array, axis, [(i, i ^ bit) for i in range(size)])
            bit *= 2
    return array


def f32_dot(a, b):
    return jnp.dot(a, b, preferred_element_type=jnp.float32)


def add_up(*arrays):
    total = arrays[0].astype(jnp.float32)
    for a in arrays[1:]:
        total = total + a.astype(jnp.float32)
    return total.astype(jnp.bfloat16)


def expert_body(block, *refs):
    rows_in = refs[:4]
    g0, g1, u0, u1, d0, d1 = refs[4:10]
    outs = refs[10:14]
    acc, hidden = refs[14:]
    count, width = rows_in[0].shape
    acc[...] = jnp.zeros_like(acc)

    @pl.loop(0, width // block)
    def _(step):
        at = pl.multiple_of(step * block, block)
        rows = jnp.concatenate([r[:, pl.ds(at, block)] for r in rows_in], axis=0)
        for i, w in enumerate((g0, g1, u0, u1)):
            acc[i] += f32_dot(rows, w[pl.ds(at, block), :])

    for i in range(2):
        hidden[i] = (jax.nn.silu(acc[i]) * acc[i + 2]).astype(jnp.bfloat16)

    @pl.loop(0, width // block)
    def _(step):
        at = pl.multiple_of(step * block, block)
        value = f32_dot(hidden[0], d0[:, pl.ds(at, block)]) + f32_dot(hidden[1], d1[:, pl.ds(at, block)])
        value = value.astype(jnp.bfloat16)
        for i, out in enumerate(outs):
            out[:, pl.ds(at, block)] = value[i * count : (i + 1) * count]


def expert_rows(rows, gates, ups, downs):
    count, width = rows[0].shape
    inner = gates[0].shape[1]
    near = pl.BlockSpec(memory_space=pltpu.VMEM)
    return pl.pallas_call(
        functools.partial(expert_body, 1024),
        in_specs=[near] * 10,
        out_specs=[near] * 4,
        out_shape=[pltpu.VMEM((count, width), jnp.bfloat16)] * 4,
        scratch_shapes=[
            pltpu.VMEM((4, 4 * count, inner), jnp.float32),
            pltpu.VMEM((2, 4 * count, inner), jnp.bfloat16),
        ],
        compiler_params=pltpu.CompilerParams(vmem_limit_bytes=20 << 20),
        cost_estimate=pl.CostEstimate(
            flops=4 * count * width * inner * 12, bytes_accessed=6 * width * inner * 2, transcendentals=0
        ),
        name="experts",
    )(*[pltpu.with_memory_space_constraint(a, pltpu.VMEM) for a in (*rows, *gates, *ups, *downs)])


def on_device(tokens, routing, router_weight, w_gate, w_up, w_down):
    token_rows = tokens[0]
    routes = routing[0]
    token_count, width = token_rows.shape
    top_count = routes.shape[1]
    experts = router_weight.shape[1]
    flight = lax.axis_size("seq") * lax.axis_size("exp")
    length = token_count * lax.axis_size("ctx") * lax.axis_size("exp")
    lanes = 128
    folds = width // lanes

    gates = (w_gate[0], swap_cores(w_gate[0]))
    ups = (w_up[0], swap_cores(w_up[0]))
    downs = (w_down[0], swap_cores(w_down[0]))

    routes_t = routes.T
    upper = (
        lax.broadcasted_iota(jnp.int32, (token_count, token_count), 0)
        < lax.broadcasted_iota(jnp.int32, (token_count, token_count), 1)
    ).astype(jnp.bfloat16)

    picks = []
    first = 0
    for n in CHUNKS:
        row = lax.broadcasted_iota(jnp.int32, (flight * n, 1), 0)
        expert_of, slot_of = row // n, first + row % n
        named = jnp.zeros((flight * n, token_count), jnp.bfloat16)
        for k in range(top_count):
            named = named + (routes_t[k][None, :] == expert_of).astype(jnp.bfloat16)
        rank = f32_dot(named, upper)
        picks.append(jnp.where(rank == slot_of.astype(jnp.float32), named, jnp.zeros((), jnp.bfloat16)))
        first += n

    received = []
    for n, pick in zip(CHUNKS, picks):
        out = f32_dot(pick, token_rows).astype(jnp.bfloat16)
        out = out.reshape(flight, n * folds, lanes)
        mine = lax.all_to_all(out, XZ, split_axis=0, concat_axis=0, tiled=True)
        received.append(mine.reshape(flight * n, width))

    late_tokens, _ = lax.optimization_barrier((token_rows, received[0]))
    scores = jax.nn.sigmoid(f32_dot(late_tokens, router_weight))
    affinity = scores / jnp.sum(scores, axis=1, keepdims=True)
    expert_iota = lax.broadcasted_iota(jnp.int32, (1, experts), 1)
    chosen = jnp.zeros((token_count, experts), jnp.float32)
    for k in range(top_count):
        chosen = chosen + (routes[:, k : k + 1] == expert_iota).astype(jnp.float32)
    gate_table = scores / jnp.sum(scores * chosen, axis=1, keepdims=True) * route_scale
    stats = jnp.stack([jnp.sum(affinity, axis=0), jnp.sum(chosen, axis=0)])
    stats = sum_all(stats)
    balance = stats[1] * (experts / (top_count * length)) * (stats[0] / length) * experts

    gathered = [[m] for m in received]
    for _ in range(3):
        for blocks in gathered:
            blocks.append(ring(blocks[-1]))

    parts = [expert_rows(blocks, gates, ups, downs) for blocks in gathered]
    moving = [ring(p[1]) for p in parts]
    for step in (2, 3):
        moving = [ring(add_up(m, p[step])) for m, p in zip(moving, parts)]

    combined = jnp.zeros((token_count, width), jnp.float32)
    for n, pick, m, p in zip(CHUNKS, picks, moving, parts):
        total = add_up(m, p[0]).reshape(flight, n * folds, lanes)
        back = lax.all_to_all(total, XZ, split_axis=0, concat_axis=0, tiled=True).reshape(flight * n, width)
        spread = (
            lax.broadcasted_iota(jnp.int32, (flight, flight * n), 0)
            == lax.broadcasted_iota(jnp.int32, (flight, flight * n), 1) // n
        ).astype(jnp.float32)
        weight = jnp.dot(gate_table[:, :flight], spread, precision=lax.Precision.HIGHEST) * pick.T.astype(jnp.float32)
        high = weight.astype(jnp.bfloat16)
        low = (weight - high.astype(jnp.float32)).astype(jnp.bfloat16)
        combined = combined + f32_dot(high, back) + f32_dot(low, back)
    return (combined.astype(jnp.bfloat16)[None], balance[None])


def solution(mesh):
    placed = (
        P("seq", ("ctx", "exp"), None),
        P("seq", ("ctx", "exp"), None),
        P(),
        P(("seq", "exp"), None, "ctx"),
        P(("seq", "exp"), None, "ctx"),
        P(("seq", "exp"), "ctx", None),
    )
    return jax.shard_map(
        on_device,
        mesh=mesh,
        in_specs=placed,
        out_specs=(P("seq", ("ctx", "exp"), None), P("seq", None)),
        check_vma=False,
    )
```
